32 devices in a mesh: genome: 8 (over z, x), anc: 4 (over y, core), trait: 1.
Axes of the slice: x: 2, y: 2, z: 4, core: 2. Of those that a mesh axis runs over, the one named last changes fastest.
Arguments:
- coefficients: float32 [4, 128, 16384], P('anc', 'trait', 'genome'), may hold values from -3 to 3
- sumstats: float32 [4, 128, 16384], P('anc', 'trait', 'genome'), may hold values from -12 to 12
- linkage: bfloat16 [4, 16384, 4096], P('anc', 'genome'), may hold values from -0.09375 to 0.09375
- band_start: int32 [4, 64], P('anc', 'genome'), may hold values from 0 to 12288, as said below
- group_ids: int32 [4, 16384], P('anc', 'genome'), may hold values from 0 to 15, never falling along the last dimension, each value on 1 to 8192 neighbouring positions
- group_weight: float32 [4, 16], P('anc'), may hold values from 0.1 to 1.5
- dosage: bfloat16 [4, 2048, 16384], P('anc', None, 'genome'), may hold values from 0 to 2
Outputs:
- updated: float32 [4, 128, 16384], P('anc', 'trait', 'genome')
- scores: float32 [4, 128, 2048], P('anc', 'trait', 'genome')
The draws below stay inside these ranges and needn't reach their ends.
Inputs may be any that keep to these rules, and one draw needn't show every extreme that they name: band_start[a, u] is the first of the 4096 consecutive SNP columns stored in linkage[a] for row block u, the SNPs u * 256 to u * 256 + 255; these columns always include the block's own SNPs. `group_ids`: group ids never fall along the SNPs of an ancestry, so each group is one run of consecutive SNPs.
All inputs are finite; a program needn't handle non-finite values.
Results may differ from the reference program's by a relative error of at most 0.003.
Values may be sent and summed in bfloat16 or wider, within the bound.
A program may use at most 128 MiB of HBM per device.

```python
import math
import jax
import jax.numpy as jnp
import numpy as np
from jax import lax

TRAITS = 128
ANC = 4
W = 4096
TILE = 256
M_DEV = 2048
PERSONS = 2048
SNPS = 16384
GROUPS = 16


def draw_band_start(key, part):
    block_count = SNPS // TILE
    spare = W - TILE
    anchors = jnp.arange(block_count, dtype=jnp.int32) * TILE
    jitter = jax.random.randint(key, (ANC, block_count), 0, spare + 1, dtype=jnp.int32)
    raw_start = anchors[None, :] - jitter
    return jnp.minimum(jnp.maximum(raw_start, 0), SNPS - W).astype(jnp.int32)


def draw_sumstats(key, part):
    block_count = SNPS // TILE
    key_noise = jax.random.fold_in(key, 11)
    key_scale = jax.random.fold_in(key, 23)
    noise = jnp.clip(jax.random.normal(key_noise, (ANC, TRAITS, SNPS), jnp.float32), -4.0, 4.0)
    block_scale = jnp.exp(jax.random.uniform(key_scale, (ANC, 1, block_count), jnp.float32, -0.69, 0.69))
    block_scale = jnp.repeat(block_scale, TILE, axis=2)
    trend = 3.0 ** (jnp.arange(SNPS, dtype=jnp.float32) / SNPS)
    return (0.5 * noise * block_scale * trend[None, None, :]).astype(jnp.float32)


def levels(key, shape, shards, smallest, largest):
    def one(axis_at, blocks):
        draws = jax.random.uniform(jax.random.fold_in(jax.random.fold_in(key, 6), axis_at), (blocks,), jnp.float32, smallest / len(shards), largest / len(shards))
        return jnp.repeat(jnp.exp(draws), shape[axis_at] // blocks).reshape((-1,) + (1,) * (len(shape) - axis_at - 1))

    level = one(*shards[0])
    for cut in shards[1:]:
        level = level * one(*cut)
    return level


def length_profile(number_of, total, most, lean):
    weights = [(1 << 20) // math.isqrt(rank ** lean) + 1 for rank in range(2, number_of + 1)]
    surplus, given = total - most - (number_of - 1), [1] * (number_of - 1)
    while surplus > 0:
        movable = [i for i in range(number_of - 1) if given[i] < most]
        mass, budget = sum([weights[i] for i in movable]), surplus
        for i in movable:
            extra = min(most - given[i], max(1, budget * weights[i] // mass), surplus)
            given[i] = given[i] + extra
            surplus = surplus - extra
    return np.array([most] + given)


def ragged_sizes(rng, count, total, bound, lean):
    if count == 2:
        one = jax.random.randint(rng, (), max(1, total - bound), min(bound, total - 1) + 1)
        return jnp.stack([one, total - one])
    tallies = jnp.asarray(length_profile(count, total, bound, lean), jnp.int32)
    couples = (count - 1) // 2
    source_of, taker = tallies[1:1 + 2 * couples:2], tallies[2:2 + 2 * couples:2]
    margin = jnp.minimum(source_of - 1, bound - taker)
    shifted = jax.random.randint(jax.random.fold_in(rng, 1), (couples,), 0, 1 << 20) % (margin + 1)
    tallies = tallies.at[1:1 + 2 * couples:2].set(source_of - shifted).at[2:2 + 2 * couples:2].set(taker + shifted)
    return tallies[jax.random.permutation(jax.random.fold_in(rng, 2), count)]


def gaussian(key, shape, scale, most, split=(), kind=jnp.bfloat16):
    entries = jax.random.normal(key, shape, jnp.float32) * scale
    if len(split) > 0:
        entries = levels(key, shape, split, -0.22, 0.18) * entries
    return jnp.clip(entries, min=-most, max=most).astype(kind)


def setup_inputs(seed: int = 0) -> dict:
    splits = jax.random.split(jax.random.key(seed), 8)
    coefficients = gaussian(splits[0], (ANC, TRAITS, SNPS), 0.5, 3.0, ((0, 4), (2, 8)), jnp.float32)
    sumstats = draw_sumstats(jax.random.fold_in(splits[7], 71), 0)
    linkage = gaussian(splits[2], (ANC, SNPS, W), W ** -0.5, 0.09375, ((0, 4), (1, 8)))
    band_start = draw_band_start(jax.random.fold_in(splits[7], 71), 0)
    group_ids = jax.vmap(lambda own: jnp.searchsorted(jnp.cumsum(ragged_sizes(own, GROUPS, SNPS, 4 * M_DEV, 2)), jnp.arange(SNPS), side="right"))(jax.random.split(splits[4], ANC)).reshape((ANC, SNPS)).astype(jnp.int32)
    group_weight = jnp.clip(jnp.exp(math.log(1.5) - 2.7080502 * jax.random.uniform(splits[5], (ANC, GROUPS), jnp.float32) ** levels(splits[5], (ANC, GROUPS), ((0, 4),), -0.2, 0.2)), 0.1, 1.5)
    dosage = jnp.clip(2.0 * jax.random.uniform(splits[6], (ANC, PERSONS, SNPS), jnp.float32) ** levels(splits[6], (ANC, PERSONS, SNPS), ((0, 4), (2, 8)), -0.2, 0.2), 0.0, 2.0).astype(jnp.bfloat16)
    return dict(coefficients=coefficients, sumstats=sumstats, linkage=linkage, band_start=band_start, group_ids=group_ids, group_weight=group_weight, dosage=dosage)


step_size = 0.5
merging = 0.5
epsilon = 1e-06

def band_apply(low_copy, band, starts):
    padded = jnp.pad(low_copy.astype(jnp.float32), ((0, 0), (W, W)))
    band_tiles = band.reshape(SNPS // TILE, TILE, W)

    def per_tile(tile_item):
        block_rows, begin_at = tile_item
        window = lax.dynamic_slice_in_dim(padded, (begin_at + W).astype(jnp.int32), W, 1)
        return jnp.dot(window, block_rows.astype(jnp.float32).T, precision=lax.Precision.HIGHEST)
    products = lax.map(per_tile, (band_tiles, starts))
    return jnp.transpose(products, (1, 0, 2)).reshape(TRAITS, SNPS)

def reference(coefficients, sumstats, linkage, band_start, group_ids, group_weight, dosage):
    mean_coef = lax.optimization_barrier(jnp.sum(coefficients, axis=0)) / ANC
    update_list = []
    score_list = []
    for ancestry in range(ANC):
        current = coefficients[ancestry]
        band_product = band_apply(current.astype(jnp.bfloat16), linkage[ancestry], band_start[ancestry])
        gradient = current + band_product - sumstats[ancestry] + merging * (current - mean_coef)
        proposal = current - step_size * gradient
        trait_total = lax.optimization_barrier(jnp.sum(proposal * proposal, axis=0))
        group_list = group_ids[ancestry]
        squares = jax.ops.segment_sum(trait_total, group_list, num_segments=GROUPS)
        counts = jax.ops.segment_sum(jnp.ones_like(trait_total), group_list, num_segments=GROUPS)
        threshold = step_size * group_weight[ancestry] * jnp.sqrt(counts * TRAITS)
        factor = jnp.maximum(0.0, 1.0 - threshold / jnp.sqrt(squares + epsilon))
        updated = proposal * factor[group_list][None, :]
        genotype = dosage[ancestry]
        scores = jnp.dot(updated.astype(jnp.bfloat16), genotype.T, preferred_element_type=jnp.float32) / math.sqrt(SNPS)
        update_list.append(updated)
        score_list.append(scores)
    return (jnp.stack(update_list), jnp.stack(score_list))
```

```python
import functools
import math

import jax
import jax.numpy as jnp
from jax import lax
from jax.experimental import pallas as pl
from jax.experimental.pallas import tpu as pltpu
from jax.sharding import PartitionSpec as P

step_size = 0.5
merging = 0.5
epsilon = 1e-06

MESH = pl.DeviceIdType.MESH
F32 = jnp.float32
BF16 = jnp.bfloat16


def step_kernel(
    sizes,
    coef_hbm, sums_hbm, link_hbm, starts_ref, ids_ref, weight_ref, dosage_hbm,
    updated_hbm, score_ref,
    coef, sums, link, dosage, low, ext, extf, peers, proposal, updated, updated_t, row,
    stats_out, stats_in, part_out, part_in,
    load_sem, link_sem, store_sem,
    halo_send, halo_recv, anc_send, anc_recv, stats_send, stats_recv, part_send, part_recv,
):
    genomes, ancs, traits_n, reach, tile, groups = sizes
    traits_here, snps = coef.shape
    width = link.shape[1]
    tiles = snps // tile
    persons_per = part_out.shape[1]
    g = lax.axis_index("genome")
    a = lax.axis_index("anc")
    t = lax.axis_index("trait")
    stat_peers = [(k, m) for m in range(traits_n) for k in range(genomes) if (k, m) != (0, 0)]

    def genome_peer(k):
        return lax.rem(g + k, genomes)

    load_coef = pltpu.make_async_copy(coef_hbm.at[0], coef, load_sem.at[0])
    load_coef.start()
    barrier = pltpu.get_barrier_semaphore()
    for k, m in stat_peers:
        pl.semaphore_signal(
            barrier, inc=1, device_id_type=MESH,
            device_id={"genome": genome_peer(k), "trait": lax.rem(t + m, traits_n)},
        )
    for k in range(1, ancs):
        pl.semaphore_signal(
            barrier, inc=1, device_id={"anc": lax.rem(a + k, ancs)}, device_id_type=MESH
        )
    load_sums = pltpu.make_async_copy(sums_hbm.at[0], sums, load_sem.at[1])
    load_sums.start()
    load_dosage = pltpu.make_async_copy(dosage_hbm.at[0], dosage, load_sem.at[2])

    def link_copy(u):
        rows = pl.ds(pl.multiple_of(u * tile, tile), tile)
        return pltpu.make_async_copy(link_hbm.at[0, rows, :], link.at[rows, :], link_sem.at[u])

    load_coef.wait()

    def own_block(u, carry):
        cols = pl.ds(pl.multiple_of(u * tile, tile), tile)
        block = coef[:, cols].astype(BF16)
        low[:, cols] = block
        flat = block.astype(F32).T
        extf[pl.ds(pl.multiple_of(reach * snps + u * tile, tile), tile), :] = flat
        ext[reach, cols, :] = flat.astype(BF16)
        return carry

    lax.fori_loop(0, tiles, own_block, 0)
    pl.semaphore_wait(barrier, len(stat_peers) + ancs - 1)

    distances = [d for far in range(1, reach + 1) for d in (far, -far)]

    def halo_copy(d):
        slot = reach - d
        return pltpu.make_async_remote_copy(
            src_ref=ext.at[reach], dst_ref=ext.at[slot],
            send_sem=halo_send.at[slot], recv_sem=halo_recv.at[slot],
            device_id={"genome": jnp.clip(g + d, 0, genomes - 1)}, device_id_type=MESH,
        )

    def in_range(p):
        return jnp.logical_and(p >= 0, p < genomes)

    for d in distances:
        @pl.when(in_range(g + d))
        def _(d=d):
            halo_copy(d).start()

    def anc_copy(k):
        return pltpu.make_async_remote_copy(
            src_ref=low, dst_ref=peers.at[k - 1],
            send_sem=anc_send.at[k - 1], recv_sem=anc_recv.at[k - 1],
            device_id={"anc": lax.rem(a + k, ancs)}, device_id_type=MESH,
        )

    for k in range(1, ancs):
        anc_copy(k).start()
    for u in range(tiles):
        link_copy(u).start()
    load_dosage.start()
    load_sums.wait()

    for d in distances:
        slot = reach - d
        chunk = 256

        @pl.when(in_range(g - d))
        def _(d=d, slot=slot):
            halo_copy(d).wait_recv()

            def widen(i, carry):
                at = pl.multiple_of(i * chunk, chunk)
                extf[pl.ds(pl.multiple_of(slot * snps + at, chunk), chunk), :] = (
                    ext[slot, pl.ds(at, chunk), :].astype(F32)
                )
                return carry

            lax.fori_loop(0, snps // chunk, widen, 0)

        @pl.when(jnp.logical_not(in_range(g - d)))
        def _(slot=slot):
            def clear(i, carry):
                at = pl.multiple_of(slot * snps + i * chunk, chunk)
                extf[pl.ds(at, chunk), :] = jnp.zeros((chunk, traits_here), F32)
                return carry

            lax.fori_loop(0, snps // chunk, clear, 0)

    for k in range(1, ancs):
        anc_copy(k).wait_recv()

    def band_tile(u, carry):
        link_copy(u).wait()
        rows = pl.ds(pl.multiple_of(u * tile, tile), tile)
        begin = jnp.clip(starts_ref[0, u] - g * snps + reach * snps, 0, extf.shape[0] - width)
        depth = 512
        total = jnp.zeros((tile, traits_here), F32)
        for c in range(0, width, depth):
            window = extf[pl.ds(begin + c, depth), :].astype(BF16)
            total = total + jnp.dot(
                link[rows, c:c + depth], window, preferred_element_type=F32
            )
        band = total.T
        current = coef[:, rows]
        mean = current
        for k in range(1, ancs):
            mean = mean + peers[k - 1, :, rows].astype(F32)
        mean = mean / ancs
        gradient = current + band - sums[:, rows] + merging * (current - mean)
        value = current - step_size * gradient
        proposal[:, rows] = value
        row[:, rows] = jnp.sum(value * value, axis=0, keepdims=True)
        return carry

    lax.fori_loop(0, tiles, band_tile, 0)

    group_of = lax.broadcasted_iota(jnp.int32, (groups, snps), 0)
    mine = group_of == ids_ref[...]
    squares = jnp.sum(jnp.where(mine, row[...], 0.0), axis=1, keepdims=True)
    counts = jnp.sum(jnp.where(mine, 1.0, 0.0), axis=1, keepdims=True)
    lane = lax.broadcasted_iota(jnp.int32, (groups, 128), 1)
    stats = jnp.where(lane == 0, squares, jnp.where(lane == 1, counts, 0.0))
    stats_out[...] = stats

    def stats_copy(i):
        k, m = stat_peers[i]
        return pltpu.make_async_remote_copy(
            src_ref=stats_out, dst_ref=stats_in.at[i],
            send_sem=stats_send.at[i], recv_sem=stats_recv.at[i],
            device_id={"genome": genome_peer(k), "trait": lax.rem(t + m, traits_n)},
            device_id_type=MESH,
        )

    for i in range(len(stat_peers)):
        stats_copy(i).start()
    load_dosage.wait()
    for i in range(len(stat_peers)):
        stats_copy(i).wait_recv()
        stats = stats + stats_in[i]
    all_squares = stats[:, 0:1]
    all_counts = stats[:, 1:2] / traits_n
    square_of = lax.broadcasted_iota(jnp.int32, (groups, groups), 0)
    lane_of = lax.broadcasted_iota(jnp.int32, (groups, groups), 1)
    weight = jnp.sum(
        jnp.where(square_of == lane_of, weight_ref[...], 0.0), axis=1, keepdims=True
    )
    threshold = step_size * weight * jnp.sqrt(all_counts * (traits_here * traits_n))
    shrink = jnp.maximum(0.0, 1.0 - threshold / jnp.sqrt(all_squares + epsilon))
    row[...] = jnp.sum(jnp.where(mine, shrink, 0.0), axis=0, keepdims=True)

    def shrink_tile(u, carry):
        cols = pl.ds(pl.multiple_of(u * tile, tile), tile)
        value = proposal[:, cols] * row[:, cols]
        updated[:, cols] = value
        updated_t[cols, :] = value.T.astype(BF16)
        return carry

    lax.fori_loop(0, tiles, shrink_tile, 0)
    store = pltpu.make_async_copy(updated, updated_hbm.at[0], store_sem)
    store.start()

    scale = 1.0 / math.sqrt(snps * genomes)

    def partial(k):
        at = pl.ds(pl.multiple_of(genome_peer(k) * persons_per, persons_per), persons_per)
        return jnp.dot(dosage[at, :], updated_t[...], preferred_element_type=F32) * scale

    def part_copy(k):
        return pltpu.make_async_remote_copy(
            src_ref=part_out.at[k - 1], dst_ref=part_in.at[k - 1],
            send_sem=part_send.at[k - 1], recv_sem=part_recv.at[k - 1],
            device_id={"genome": genome_peer(k)}, device_id_type=MESH,
        )

    def send_part(k, carry):
        part_out[k - 1] = partial(k).astype(BF16)
        part_copy(k).start()
        return carry

    lax.fori_loop(1, genomes, send_part, 0)

    def add_part(k, total):
        part_copy(k).wait_recv()
        return total + part_in[k - 1].astype(F32)

    score_ref[0] = lax.fori_loop(1, genomes, add_part, partial(0)).T

    store.wait()
    for d in distances:
        @pl.when(in_range(g + d))
        def _(d=d):
            halo_copy(d).wait_send()
    for k in range(1, ancs):
        anc_copy(k).wait_send()
    for i in range(len(stat_peers)):
        stats_copy(i).wait_send()

    def sent_part(k, carry):
        part_copy(k).wait_send()
        return carry

    lax.fori_loop(1, genomes, sent_part, 0)


def per_device(coefficients, sumstats, linkage, band_start, group_ids, group_weight, dosage):
    _, traits_here, snps = coefficients.shape
    width = linkage.shape[2]
    genomes = lax.axis_size("genome")
    ancs = lax.axis_size("anc")
    traits_n = lax.axis_size("trait")
    persons = dosage.shape[1]
    persons_per = persons // genomes
    groups = group_weight.shape[1]
    reach = -(-width // snps)
    tile = snps // band_start.shape[1]
    slots = 2 * reach + 1
    stat_n = genomes * traits_n - 1
    sizes = (genomes, ancs, traits_n, reach, tile, groups)
    anyspace = pl.BlockSpec(memory_space=pl.ANY)
    vmem = pl.BlockSpec(memory_space=pltpu.VMEM)
    smem = pl.BlockSpec(memory_space=pltpu.SMEM)
    dma = pltpu.SemaphoreType.DMA
    return pl.pallas_call(
        functools.partial(step_kernel, sizes),
        out_shape=(
            jax.ShapeDtypeStruct((1, traits_here, snps), F32),
            jax.ShapeDtypeStruct((1, traits_here, persons_per), F32),
        ),
        in_specs=[anyspace, anyspace, anyspace, smem, vmem, vmem, anyspace],
        out_specs=(anyspace, vmem),
        scratch_shapes=[
            pltpu.VMEM((traits_here, snps), F32),
            pltpu.VMEM((traits_here, snps), F32),
            pltpu.VMEM((snps, width), BF16),
            pltpu.VMEM((persons, snps), BF16),
            pltpu.VMEM((traits_here, snps), BF16),
            pltpu.VMEM((slots, snps, traits_here), BF16),
            pltpu.VMEM((slots * snps, traits_here), F32),
            pltpu.VMEM((ancs - 1, traits_here, snps), BF16),
            pltpu.VMEM((traits_here, snps), F32),
            pltpu.VMEM((traits_here, snps), F32),
            pltpu.VMEM((snps, traits_here), BF16),
            pltpu.VMEM((1, snps), F32),
            pltpu.VMEM((groups, 128), F32),
            pltpu.VMEM((stat_n, groups, 128), F32),
            pltpu.VMEM((genomes - 1, persons_per, traits_here), BF16),
            pltpu.VMEM((genomes - 1, persons_per, traits_here), BF16),
            dma((3,)), dma((snps // tile,)), dma,
            dma((slots,)), dma((slots,)), dma((ancs - 1,)), dma((ancs - 1,)),
            dma((stat_n,)), dma((stat_n,)), dma((genomes - 1,)), dma((genomes - 1,)),
        ],
        compiler_params=pltpu.CompilerParams(
            collective_id=0, has_side_effects=True, vmem_limit_bytes=56 * 1024 * 1024
        ),
    )(coefficients, sumstats, linkage, band_start, group_ids, group_weight, dosage)


def solution(mesh):
    in_specs = (
        P("anc", "trait", "genome"),
        P("anc", "trait", "genome"),
        P("anc", "genome", None),
        P("anc", "genome"),
        P("anc", "genome"),
        P("anc", None),
        P("anc", None, "genome"),
    )
    out_specs = (P("anc", "trait", "genome"), P("anc", "trait", "genome"))
    return jax.shard_map(
        per_device, mesh=mesh, in_specs=in_specs, out_specs=out_specs, check_vma=False
    )
```

```python
import functools
import math

import jax
import jax.numpy as jnp
from jax import lax
from jax.experimental import pallas as pl
from jax.experimental.pallas import tpu as pltpu
from jax.sharding import PartitionSpec as P

step_size = 0.5
merging = 0.5
epsilon = 1e-06

MESH = pl.DeviceIdType.MESH
F32 = jnp.float32
BF16 = jnp.bfloat16


def step_kernel(
    sizes,
    coef_hbm, sums_hbm, link_hbm, starts_ref, ids_ref, weight_ref, dosage_hbm,
    updated_hbm, score_ref,
    coef, sums, link, dosage, low, ext, extf, peers, proposal, updated, updated_t, row,
    stats_out, stats_in, part_out, part_in,
    load_sem, link_sem, store_sem,
    halo_send, halo_recv, anc_send, anc_recv, stats_send, stats_recv, part_send, part_recv,
):
    genomes, ancs, traits_n, reach, tile, groups = sizes
    traits_here, snps = coef.shape
    width = link.shape[1]
    tiles = snps // tile
    persons_per = part_out.shape[1]
    g = lax.axis_index("genome")
    a = lax.axis_index("anc")
    t = lax.axis_index("trait")
    stat_peers = [(k, m) for m in range(traits_n) for k in range(genomes) if (k, m) != (0, 0)]

    def genome_peer(k):
        return lax.rem(g + k, genomes)

    load_coef = pltpu.make_async_copy(coef_hbm.at[0], coef, load_sem.at[0])
    load_coef.start()
    barrier = pltpu.get_barrier_semaphore()
    for k, m in stat_peers:
        pl.semaphore_signal(
            barrier, inc=1, device_id_type=MESH,
            device_id={"genome": genome_peer(k), "trait": lax.rem(t + m, traits_n)},
        )
    for k in range(1, ancs):
        pl.semaphore_signal(
            barrier, inc=1, device_id={"anc": lax.rem(a + k, ancs)}, device_id_type=MESH
        )
    load_sums = pltpu.make_async_copy(sums_hbm.at[0], sums, load_sem.at[1])
    load_sums.start()
    load_dosage = pltpu.make_async_copy(dosage_hbm.at[0], dosage, load_sem.at[2])

    def link_copy(u):
        rows = pl.ds(pl.multiple_of(u * tile, tile), tile)
        return pltpu.make_async_copy(link_hbm.at[0, rows, :], link.at[rows, :], link_sem.at[u])

    load_coef.wait()

    half = snps // 2
    even = 1 - 2 * lax.rem(g, 2)
    near, far, across = g + even, g + 2 * even, g - even

    def in_range(p):
        return jnp.logical_and(p >= 0, p < genomes)

    def own_block(u, carry):
        cols = pl.ds(pl.multiple_of(u * tile, tile), tile)
        block = coef[:, cols].astype(BF16)
        low[:, cols] = block
        flat = block.astype(F32).T
        extf[pl.ds(pl.multiple_of(reach * snps + u * tile, tile), tile), :] = flat
        ext[reach, cols, :] = flat.astype(BF16)
        return carry

    def halo_copy(src_slot, dst_slot, h, peer, send):
        rows = pl.ds(h * half, half)
        return pltpu.make_async_remote_copy(
            src_ref=ext.at[src_slot, rows, :], dst_ref=ext.at[dst_slot, rows, :],
            send_sem=halo_send.at[send], recv_sem=halo_recv.at[dst_slot, h],
            device_id={"genome": jnp.clip(peer, 0, genomes - 1)}, device_id_type=MESH,
        )

    def near_copy(h):
        return halo_copy(reach, reach - even, h, near, h)

    def far_copy(d, h):
        return halo_copy(reach, reach - d, h, g + d, (2 if d > 0 else 4) + h)

    def relay_far():
        return halo_copy(reach + even, reach - even, 0, far, 6)

    def relay_near():
        return halo_copy(reach + 2 * even, reach + even, 1, near, 7)

    def arrived(slot, h):
        halo_copy(reach, slot, h, near, 0).wait_recv()

    def anc_copy(k):
        return pltpu.make_async_remote_copy(
            src_ref=low, dst_ref=peers.at[k - 1],
            send_sem=anc_send.at[k - 1], recv_sem=anc_recv.at[k - 1],
            device_id={"anc": lax.rem(a + k, ancs)}, device_id_type=MESH,
        )

    def far_each(h):
        for d in (2, -2):
            @pl.when(in_range(g + d))
            def _(d=d):
                far_copy(d, h).start()

    lax.fori_loop(0, tiles // 2, own_block, 0)
    pl.semaphore_wait(barrier, len(stat_peers) + ancs - 1)
    near_copy(0).start()
    lax.fori_loop(tiles // 2, tiles, own_block, 0)
    far_each(1)
    near_copy(1).start()
    far_each(0)
    for k in range(1, ancs):
        anc_copy(k).start()
    for u in range(tiles):
        link_copy(u).start()
    load_dosage.start()

    chunk = 256

    def widen(slot, h):
        def piece(i, carry):
            at = pl.multiple_of(h * half + i * chunk, chunk)
            extf[pl.ds(pl.multiple_of(slot * snps + at, chunk), chunk), :] = (
                ext[slot, pl.ds(at, chunk), :].astype(F32)
            )
            return carry

        lax.fori_loop(0, half // chunk, piece, 0)

    for d in (-2, -1, 1, 2):
        @pl.when(jnp.logical_not(in_range(g + d)))
        def _(slot=reach + d):
            def clear(i, carry):
                at = pl.multiple_of(slot * snps + i * chunk, chunk)
                extf[pl.ds(at, chunk), :] = jnp.zeros((chunk, traits_here), F32)
                return carry

            lax.fori_loop(0, snps // chunk, clear, 0)

    arrived(reach + even, 0)

    @pl.when(in_range(far))
    def _():
        relay_far().start()
        arrived(reach + 2 * even, 1)
        relay_near().start()

    widen(reach + even, 0)

    @pl.when(in_range(far))
    def _():
        widen(reach + 2 * even, 1)

    @pl.when(in_range(g - 2 * even))
    def _():
        arrived(reach - 2 * even, 1)
        widen(reach - 2 * even, 1)

    arrived(reach + even, 1)
    widen(reach + even, 1)

    @pl.when(in_range(far))
    def _():
        arrived(reach + 2 * even, 0)
        widen(reach + 2 * even, 0)

    @pl.when(in_range(g - 2 * even))
    def _():
        arrived(reach - 2 * even, 0)
        widen(reach - 2 * even, 0)

    @pl.when(in_range(across))
    def _():
        for h in range(2):
            arrived(reach - even, h)
            widen(reach - even, h)

    load_sums.wait()

    def band_tile(u, carry):
        link_copy(u).wait()
        rows = pl.ds(pl.multiple_of(u * tile, tile), tile)
        begin = jnp.clip(starts_ref[0, u] - g * snps + reach * snps, 0, extf.shape[0] - width)
        depth = 512
        total = jnp.zeros((tile, traits_here), F32)
        for c in range(0, width, depth):
            window = extf[pl.ds(begin + c, depth), :].astype(BF16)
            total = total + jnp.dot(
                link[rows, c:c + depth], window, preferred_element_type=F32
            )
        band = total.T
        current = coef[:, rows]
        proposal[:, rows] = current + band - sums[:, rows]
        return carry

    lax.fori_loop(0, tiles, band_tile, 0)
    for k in range(1, ancs):
        anc_copy(k).wait_recv()

    def propose(u, carry):
        cols = pl.ds(pl.multiple_of(u * tile, tile), tile)
        current = coef[:, cols]
        mean = current
        for k in range(1, ancs):
            mean = mean + peers[k - 1, :, cols].astype(F32)
        mean = mean / ancs
        gradient = proposal[:, cols] + merging * (current - mean)
        value = current - step_size * gradient
        proposal[:, cols] = value
        row[:, cols] = jnp.sum(value * value, axis=0, keepdims=True)
        return carry

    lax.fori_loop(0, tiles, propose, 0)

    group_of = lax.broadcasted_iota(jnp.int32, (groups, snps), 0)
    mine = group_of == ids_ref[...]
    squares = jnp.sum(jnp.where(mine, row[...], 0.0), axis=1, keepdims=True)
    counts = jnp.sum(jnp.where(mine, 1.0, 0.0), axis=1, keepdims=True)
    lane = lax.broadcasted_iota(jnp.int32, (groups, 128), 1)
    stats = jnp.where(lane == 0, squares, jnp.where(lane == 1, counts, 0.0))
    stats_out[...] = stats

    def stats_copy(i):
        k, m = stat_peers[i]
        return pltpu.make_async_remote_copy(
            src_ref=stats_out, dst_ref=stats_in.at[i],
            send_sem=stats_send.at[i], recv_sem=stats_recv.at[i],
            device_id={"genome": genome_peer(k), "trait": lax.rem(t + m, traits_n)},
            device_id_type=MESH,
        )

    for i in range(len(stat_peers)):
        stats_copy(i).start()
    load_dosage.wait()
    for i in range(len(stat_peers)):
        stats_copy(i).wait_recv()
        stats = stats + stats_in[i]
    all_squares = stats[:, 0:1]
    all_counts = stats[:, 1:2] / traits_n
    square_of = lax.broadcasted_iota(jnp.int32, (groups, groups), 0)
    lane_of = lax.broadcasted_iota(jnp.int32, (groups, groups), 1)
    weight = jnp.sum(
        jnp.where(square_of == lane_of, weight_ref[...], 0.0), axis=1, keepdims=True
    )
    threshold = step_size * weight * jnp.sqrt(all_counts * (traits_here * traits_n))
    shrink = jnp.maximum(0.0, 1.0 - threshold / jnp.sqrt(all_squares + epsilon))
    row[...] = jnp.sum(jnp.where(mine, shrink, 0.0), axis=0, keepdims=True)

    def shrink_tile(u, carry):
        cols = pl.ds(pl.multiple_of(u * tile, tile), tile)
        value = proposal[:, cols] * row[:, cols]
        updated[:, cols] = value
        updated_t[cols, :] = value.T.astype(BF16)
        return carry

    lax.fori_loop(0, tiles, shrink_tile, 0)
    store = pltpu.make_async_copy(updated, updated_hbm.at[0], store_sem)
    store.start()

    scale = 1.0 / math.sqrt(snps * genomes)

    def partial(k):
        at = pl.ds(pl.multiple_of(genome_peer(k) * persons_per, persons_per), persons_per)
        return jnp.dot(dosage[at, :], updated_t[...], preferred_element_type=F32) * scale

    def part_copy(k):
        return pltpu.make_async_remote_copy(
            src_ref=part_out.at[k - 1], dst_ref=part_in.at[k - 1],
            send_sem=part_send.at[k - 1], recv_sem=part_recv.at[k - 1],
            device_id={"genome": genome_peer(k)}, device_id_type=MESH,
        )

    def send_part(k, carry):
        part_out[k - 1] = partial(k).astype(BF16)
        part_copy(k).start()
        return carry

    lax.fori_loop(1, genomes, send_part, 0)

    def add_part(k, total):
        part_copy(k).wait_recv()
        return total + part_in[k - 1].astype(F32)

    score_ref[0] = lax.fori_loop(1, genomes, add_part, partial(0)).T

    store.wait()
    for h in range(2):
        near_copy(h).wait_send()
        for d in (2, -2):
            @pl.when(in_range(g + d))
            def _(d=d, h=h):
                far_copy(d, h).wait_send()

    @pl.when(in_range(far))
    def _():
        relay_far().wait_send()
        relay_near().wait_send()

    for k in range(1, ancs):
        anc_copy(k).wait_send()
    for i in range(len(stat_peers)):
        stats_copy(i).wait_send()

    def sent_part(k, carry):
        part_copy(k).wait_send()
        return carry

    lax.fori_loop(1, genomes, sent_part, 0)


def per_device(coefficients, sumstats, linkage, band_start, group_ids, group_weight, dosage):
    _, traits_here, snps = coefficients.shape
    width = linkage.shape[2]
    genomes = lax.axis_size("genome")
    ancs = lax.axis_size("anc")
    traits_n = lax.axis_size("trait")
    persons = dosage.shape[1]
    persons_per = persons // genomes
    groups = group_weight.shape[1]
    reach = -(-width // snps)
    assert reach == 2 and genomes % 2 == 0 and coefficients.shape[0] == 1
    tile = snps // band_start.shape[1]
    slots = 2 * reach + 1
    stat_n = genomes * traits_n - 1
    sizes = (genomes, ancs, traits_n, reach, tile, groups)
    anyspace = pl.BlockSpec(memory_space=pl.ANY)
    vmem = pl.BlockSpec(memory_space=pltpu.VMEM)
    smem = pl.BlockSpec(memory_space=pltpu.SMEM)
    dma = pltpu.SemaphoreType.DMA
    return pl.pallas_call(
        functools.partial(step_kernel, sizes),
        out_shape=(
            jax.ShapeDtypeStruct((1, traits_here, snps), F32),
            jax.ShapeDtypeStruct((1, traits_here, persons_per), F32),
        ),
        in_specs=[anyspace, anyspace, anyspace, smem, vmem, vmem, anyspace],
        out_specs=(anyspace, vmem),
        scratch_shapes=[
            pltpu.VMEM((traits_here, snps), F32),
            pltpu.VMEM((traits_here, snps), F32),
            pltpu.VMEM((snps, width), BF16),
            pltpu.VMEM((persons, snps), BF16),
            pltpu.VMEM((traits_here, snps), BF16),
            pltpu.VMEM((slots, snps, traits_here), BF16),
            pltpu.VMEM((slots * snps, traits_here), F32),
            pltpu.VMEM((ancs - 1, traits_here, snps), BF16),
            pltpu.VMEM((traits_here, snps), F32),
            pltpu.VMEM((traits_here, snps), F32),
            pltpu.VMEM((snps, traits_here), BF16),
            pltpu.VMEM((1, snps), F32),
            pltpu.VMEM((groups, 128), F32),
            pltpu.VMEM((stat_n, groups, 128), F32),
            pltpu.VMEM((genomes - 1, persons_per, traits_here), BF16),
            pltpu.VMEM((genomes - 1, persons_per, traits_here), BF16),
            dma((3,)), dma((snps // tile,)), dma,
            dma((8,)), dma((slots, 2)), dma((ancs - 1,)), dma((ancs - 1,)),
            dma((stat_n,)), dma((stat_n,)), dma((genomes - 1,)), dma((genomes - 1,)),
        ],
        compiler_params=pltpu.CompilerParams(
            collective_id=0, has_side_effects=True, vmem_limit_bytes=56 * 1024 * 1024
        ),
    )(coefficients, sumstats, linkage, band_start, group_ids, group_weight, dosage)


def solution(mesh):
    in_specs = (
        P("anc", "trait", "genome"),
        P("anc", "trait", "genome"),
        P("anc", "genome", None),
        P("anc", "genome"),
        P("anc", "genome"),
        P("anc", None),
        P("anc", None, "genome"),
    )
    out_specs = (P("anc", "trait", "genome"), P("anc", "trait", "genome"))
    return jax.shard_map(
        per_device, mesh=mesh, in_specs=in_specs, out_specs=out_specs, check_vma=False
    )
```

```python
import functools
import math

import jax
import jax.numpy as jnp
from jax import lax
from jax.experimental import pallas as pl
from jax.experimental.pallas import tpu as pltpu
from jax.sharding import PartitionSpec as P

step_size = 0.5
merging = 0.5
epsilon = 1e-06

MESH = pl.DeviceIdType.MESH
F32 = jnp.float32
BF16 = jnp.bfloat16


def step_kernel(
    sizes,
    coef_hbm, sums_hbm, link_hbm, starts_hbm, ids_hbm, weight_hbm, dosage_hbm,
    updated_hbm, score_ref,
    coef, sums, link, starts_ref, ids_ref, weight_ref, dosage, low, ext, extf, peers, proposal, updated, updated_t, row,
    stats_out, stats_in, side_out, side_in, part_out, part_in,
    load_sem, link_sem, store_sem,
    halo_send, halo_recv, anc_send, anc_recv, stats_send, stats_recv, side_send, side_recv, part_send, part_recv,
):
    genomes, ancs, traits_n, reach, tile, groups = sizes
    traits_here, snps = coef.shape
    width = link.shape[1]
    tiles = snps // tile
    persons_per = part_out.shape[1]
    g = lax.axis_index("genome")
    a = lax.axis_index("anc")
    t = lax.axis_index("trait")
    stat_peers = [(k, m) for m in range(traits_n) for k in range(genomes) if (k, m) != (0, 0)]

    def genome_peer(k):
        return lax.rem(g + k, genomes)

    load_coef = pltpu.make_async_copy(coef_hbm.at[0], coef, load_sem.at[0])
    load_coef.start()
    barrier = pltpu.get_barrier_semaphore()
    for k, m in stat_peers:
        pl.semaphore_signal(
            barrier, inc=1, device_id_type=MESH,
            device_id={"genome": genome_peer(k), "trait": lax.rem(t + m, traits_n)},
        )
    for k in range(1, ancs):
        pl.semaphore_signal(
            barrier, inc=1, device_id={"anc": lax.rem(a + k, ancs)}, device_id_type=MESH
        )
    load_sums = pltpu.make_async_copy(sums_hbm.at[0], sums, load_sem.at[1])
    load_sums.start()
    load_small = [
        pltpu.make_async_copy(starts_hbm, starts_ref, load_sem.at[3]),
        pltpu.make_async_copy(ids_hbm, ids_ref, load_sem.at[4]),
        pltpu.make_async_copy(weight_hbm, weight_ref, load_sem.at[5]),
    ]
    for load in load_small:
        load.start()
    load_dosage = pltpu.make_async_copy(dosage_hbm.at[0], dosage, load_sem.at[2])

    def link_copy(u):
        rows = pl.ds(pl.multiple_of(u * tile, tile), tile)
        return pltpu.make_async_copy(link_hbm.at[0, rows, :], link.at[rows, :], link_sem.at[u])

    load_coef.wait()

    half = snps // 2
    even = 1 - 2 * lax.rem(g, 2)
    near, far, across = g + even, g + 2 * even, g - even

    def in_range(p):
        return jnp.logical_and(p >= 0, p < genomes)

    def own_block(u, carry):
        cols = pl.ds(pl.multiple_of(u * tile, tile), tile)
        block = coef[:, cols].astype(BF16)
        low[:, cols] = block
        flat = block.astype(F32).T
        extf[pl.ds(pl.multiple_of(reach * snps + u * tile, tile), tile), :] = flat
        ext[reach, cols, :] = flat.astype(BF16)
        return carry

    def halo_copy(src_slot, dst_slot, h, peer, send):
        rows = pl.ds(h * half, half)
        return pltpu.make_async_remote_copy(
            src_ref=ext.at[src_slot, rows, :], dst_ref=ext.at[dst_slot, rows, :],
            send_sem=halo_send.at[send], recv_sem=halo_recv.at[dst_slot, h],
            device_id={"genome": jnp.clip(peer, 0, genomes - 1)}, device_id_type=MESH,
        )

    def near_copy(h):
        return halo_copy(reach, reach - even, h, near, h)

    def far_copy(d, h):
        return halo_copy(reach, reach - d, h, g + d, (2 if d > 0 else 4) + h)

    def relay_far():
        return halo_copy(reach + even, reach - even, 0, far, 6)

    def relay_near():
        return halo_copy(reach + 2 * even, reach + even, 1, near, 7)

    def arrived(slot, h):
        halo_copy(reach, slot, h, near, 0).wait_recv()

    def anc_copy(k):
        return pltpu.make_async_remote_copy(
            src_ref=low, dst_ref=peers.at[k - 1],
            send_sem=anc_send.at[k - 1], recv_sem=anc_recv.at[k - 1],
            device_id={"anc": lax.rem(a + k, ancs)}, device_id_type=MESH,
        )

    def far_each(h):
        for d in (2, -2):
            @pl.when(in_range(g + d))
            def _(d=d):
                far_copy(d, h).start()

    lax.fori_loop(0, tiles // 2, own_block, 0)
    pl.semaphore_wait(barrier, len(stat_peers) + ancs - 1)
    near_copy(0).start()
    lax.fori_loop(tiles // 2, tiles, own_block, 0)
    far_each(1)
    near_copy(1).start()
    far_each(0)
    for k in range(1, ancs):
        anc_copy(k).start()
    for u in range(tiles):
        link_copy(u).start()
    load_dosage.start()

    chunk = 256

    def widen(slot, h):
        def piece(i, carry):
            at = pl.multiple_of(h * half + i * chunk, chunk)
            extf[pl.ds(pl.multiple_of(slot * snps + at, chunk), chunk), :] = (
                ext[slot, pl.ds(at, chunk), :].astype(F32)
            )
            return carry

        lax.fori_loop(0, half // chunk, piece, 0)

    for d in (-2, -1, 1, 2):
        @pl.when(jnp.logical_not(in_range(g + d)))
        def _(slot=reach + d):
            def clear(i, carry):
                at = pl.multiple_of(slot * snps + i * chunk, chunk)
                extf[pl.ds(at, chunk), :] = jnp.zeros((chunk, traits_here), F32)
                return carry

            lax.fori_loop(0, snps // chunk, clear, 0)

    arrived(reach + even, 0)

    @pl.when(in_range(far))
    def _():
        relay_far().start()
        arrived(reach + 2 * even, 1)
        relay_near().start()

    widen(reach + even, 0)

    @pl.when(in_range(far))
    def _():
        widen(reach + 2 * even, 1)

    @pl.when(in_range(g - 2 * even))
    def _():
        arrived(reach - 2 * even, 1)
        widen(reach - 2 * even, 1)

    arrived(reach + even, 1)
    widen(reach + even, 1)

    @pl.when(in_range(far))
    def _():
        arrived(reach + 2 * even, 0)
        widen(reach + 2 * even, 0)

    @pl.when(in_range(g - 2 * even))
    def _():
        arrived(reach - 2 * even, 0)
        widen(reach - 2 * even, 0)

    @pl.when(in_range(across))
    def _():
        for h in range(2):
            arrived(reach - even, h)
            widen(reach - even, h)

    load_sums.wait()
    for load in load_small:
        load.wait()

    def band_tile(u, carry):
        link_copy(u).wait()
        rows = pl.ds(pl.multiple_of(u * tile, tile), tile)
        begin = jnp.clip(starts_ref[0, u] - g * snps + reach * snps, 0, extf.shape[0] - width)
        depth = 512
        total = jnp.zeros((tile, traits_here), F32)
        for c in range(0, width, depth):
            window = extf[pl.ds(begin + c, depth), :].astype(BF16)
            total = total + jnp.dot(
                link[rows, c:c + depth], window, preferred_element_type=F32
            )
        band = total.T
        current = coef[:, rows]
        proposal[:, rows] = current + band - sums[:, rows]
        return carry

    lax.fori_loop(0, tiles, band_tile, 0)
    for k in range(1, ancs):
        anc_copy(k).wait_recv()

    def propose(u, carry):
        cols = pl.ds(pl.multiple_of(u * tile, tile), tile)
        current = coef[:, cols]
        mean = current
        for k in range(1, ancs):
            mean = mean + peers[k - 1, :, cols].astype(F32)
        mean = mean / ancs
        gradient = proposal[:, cols] + merging * (current - mean)
        value = current - step_size * gradient
        proposal[:, cols] = value
        row[:, cols] = jnp.sum(value * value, axis=0, keepdims=True)
        return carry

    lax.fori_loop(0, tiles, propose, 0)

    group_of = lax.broadcasted_iota(jnp.int32, (groups, snps), 0)
    mine = group_of == ids_ref[...]
    squares = jnp.sum(jnp.where(mine, row[...], 0.0), axis=1, keepdims=True)
    counts = jnp.sum(jnp.where(mine, 1.0, 0.0), axis=1, keepdims=True)
    lane = lax.broadcasted_iota(jnp.int32, (groups, 128), 1)
    stats = jnp.where(lane == 0, squares, jnp.where(lane == 1, counts, 0.0))
    stats_out[...] = stats

    def stats_copy(i):
        k, m = stat_peers[i]
        return pltpu.make_async_remote_copy(
            src_ref=stats_out, dst_ref=stats_in.at[i],
            send_sem=stats_send.at[i], recv_sem=stats_recv.at[i],
            device_id={"genome": genome_peer(k), "trait": lax.rem(t + m, traits_n)},
            device_id_type=MESH,
        )

    for i in range(len(stat_peers)):
        stats_copy(i).start()
    load_dosage.wait()
    for i in range(len(stat_peers)):
        stats_copy(i).wait_recv()
        stats = stats + stats_in[i]
    all_squares = stats[:, 0:1]
    all_counts = stats[:, 1:2] / traits_n
    square_of = lax.broadcasted_iota(jnp.int32, (groups, groups), 0)
    lane_of = lax.broadcasted_iota(jnp.int32, (groups, groups), 1)
    weight = jnp.sum(
        jnp.where(square_of == lane_of, weight_ref[...], 0.0), axis=1, keepdims=True
    )
    threshold = step_size * weight * jnp.sqrt(all_counts * (traits_here * traits_n))
    shrink = jnp.maximum(0.0, 1.0 - threshold / jnp.sqrt(all_squares + epsilon))
    row[...] = jnp.sum(jnp.where(mine, shrink, 0.0), axis=0, keepdims=True)

    def shrink_tile(u, carry):
        cols = pl.ds(pl.multiple_of(u * tile, tile), tile)
        value = proposal[:, cols] * row[:, cols]
        updated[:, cols] = value
        updated_t[cols, :] = value.T.astype(BF16)
        return carry

    lax.fori_loop(0, tiles, shrink_tile, 0)
    store = pltpu.make_async_copy(updated, updated_hbm.at[0], store_sem)
    store.start()

    scale = 1.0 / math.sqrt(snps * genomes)

    pairs = genomes // 2
    own_side, other_side = lax.rem(g, 2), lax.rem(near, 2)

    def pair_at(i):
        k = pairs // 2 + (1 - 2 * lax.rem(i, 2)) * ((i + 1) // 2)
        return lax.rem(g // 2 + k + pairs, pairs)

    def partial(person):
        at = pl.ds(pl.multiple_of(person * persons_per, persons_per), persons_per)
        return jnp.dot(dosage[at, :], updated_t[...], preferred_element_type=F32) * scale

    def side_copy(i):
        return pltpu.make_async_remote_copy(
            src_ref=side_out.at[i], dst_ref=side_in.at[i],
            send_sem=side_send.at[i], recv_sem=side_recv.at[i],
            device_id={"genome": near}, device_id_type=MESH,
        )

    def part_copy(i):
        return pltpu.make_async_remote_copy(
            src_ref=part_out.at[i], dst_ref=part_in.at[i],
            send_sem=part_send.at[i], recv_sem=part_recv.at[i],
            device_id={"genome": 2 * pair_at(i) + own_side}, device_id_type=MESH,
        )

    def send_side(i, carry):
        side_out[i] = partial(2 * pair_at(i) + other_side).astype(BF16)
        side_copy(i).start()
        return carry

    def pair_sum(i):
        mine_here = partial(2 * pair_at(i) + own_side)
        side_copy(i).wait_recv()
        return mine_here + side_in[i].astype(F32)

    def send_part(i, carry):
        part_out[i] = pair_sum(i).astype(BF16)
        part_copy(i).start()
        return carry

    lax.fori_loop(0, pairs, send_side, 0)
    lax.fori_loop(0, pairs - 1, send_part, 0)

    def add_part(i, total):
        part_copy(i).wait_recv()
        return total + part_in[i].astype(F32)

    score_ref[0] = lax.fori_loop(0, pairs - 1, add_part, pair_sum(pairs - 1)).T

    store.wait()
    for h in range(2):
        near_copy(h).wait_send()
        for d in (2, -2):
            @pl.when(in_range(g + d))
            def _(d=d, h=h):
                far_copy(d, h).wait_send()

    @pl.when(in_range(far))
    def _():
        relay_far().wait_send()
        relay_near().wait_send()

    for k in range(1, ancs):
        anc_copy(k).wait_send()
    for i in range(len(stat_peers)):
        stats_copy(i).wait_send()

    def sent_side(i, carry):
        side_copy(i).wait_send()
        return carry

    def sent_part(i, carry):
        part_copy(i).wait_send()
        return carry

    lax.fori_loop(0, pairs, sent_side, 0)
    lax.fori_loop(0, pairs - 1, sent_part, 0)


def per_device(coefficients, sumstats, linkage, band_start, group_ids, group_weight, dosage):
    _, traits_here, snps = coefficients.shape
    width = linkage.shape[2]
    genomes = lax.axis_size("genome")
    ancs = lax.axis_size("anc")
    traits_n = lax.axis_size("trait")
    persons = dosage.shape[1]
    persons_per = persons // genomes
    groups = group_weight.shape[1]
    reach = -(-width // snps)
    assert reach == 2 and genomes % 2 == 0 and coefficients.shape[0] == 1
    tile = snps // band_start.shape[1]
    slots = 2 * reach + 1
    pairs = genomes // 2
    stat_n = genomes * traits_n - 1
    sizes = (genomes, ancs, traits_n, reach, tile, groups)
    anyspace = pl.BlockSpec(memory_space=pl.ANY)
    hbm = pl.BlockSpec(memory_space=pltpu.HBM)
    vmem = pl.BlockSpec(memory_space=pltpu.VMEM)
    dma = pltpu.SemaphoreType.DMA
    return pl.pallas_call(
        functools.partial(step_kernel, sizes),
        out_shape=(
            jax.ShapeDtypeStruct((1, traits_here, snps), F32),
            jax.ShapeDtypeStruct((1, traits_here, persons_per), F32),
        ),
        in_specs=[hbm] * 7,
        out_specs=(anyspace, vmem),
        scratch_shapes=[
            pltpu.VMEM((traits_here, snps), F32),
            pltpu.VMEM((traits_here, snps), F32),
            pltpu.VMEM((snps, width), BF16),
            pltpu.SMEM(band_start.shape, jnp.int32),
            pltpu.VMEM(group_ids.shape, jnp.int32),
            pltpu.VMEM(group_weight.shape, F32),
            pltpu.VMEM((persons, snps), BF16),
            pltpu.VMEM((traits_here, snps), BF16),
            pltpu.VMEM((slots, snps, traits_here), BF16),
            pltpu.VMEM((slots * snps, traits_here), F32),
            pltpu.VMEM((ancs - 1, traits_here, snps), BF16),
            pltpu.VMEM((traits_here, snps), F32),
            pltpu.VMEM((traits_here, snps), F32),
            pltpu.VMEM((snps, traits_here), BF16),
            pltpu.VMEM((1, snps), F32),
            pltpu.VMEM((groups, 128), F32),
            pltpu.VMEM((stat_n, groups, 128), F32),
            pltpu.VMEM((pairs, persons_per, traits_here), BF16),
            pltpu.VMEM((pairs, persons_per, traits_here), BF16),
            pltpu.VMEM((pairs - 1, persons_per, traits_here), BF16),
            pltpu.VMEM((pairs - 1, persons_per, traits_here), BF16),
            dma((6,)), dma((snps // tile,)), dma,
            dma((8,)), dma((slots, 2)), dma((ancs - 1,)), dma((ancs - 1,)),
            dma((stat_n,)), dma((stat_n,)), dma((pairs,)), dma((pairs,)), dma((pairs - 1,)), dma((pairs - 1,)),
        ],
        compiler_params=pltpu.CompilerParams(
            collective_id=0, has_side_effects=True, vmem_limit_bytes=52 * 1024 * 1024
        ),
    )(coefficients, sumstats, linkage, band_start, group_ids, group_weight, dosage)


def solution(mesh):
    in_specs = (
        P("anc", "trait", "genome"),
        P("anc", "trait", "genome"),
        P("anc", "genome", None),
        P("anc", "genome"),
        P("anc", "genome"),
        P("anc", None),
        P("anc", None, "genome"),
    )
    out_specs = (P("anc", "trait", "genome"), P("anc", "trait", "genome"))
    return jax.shard_map(
        per_device, mesh=mesh, in_specs=in_specs, out_specs=out_specs, check_vma=False
    )
```

```python
import functools
import math

import jax
import jax.numpy as jnp
from jax import lax
from jax.experimental import pallas as pl
from jax.experimental.pallas import tpu as pltpu
from jax.sharding import PartitionSpec as P

step_size = 0.5
merging = 0.5
epsilon = 1e-06

MESH = pl.DeviceIdType.MESH
F32 = jnp.float32
BF16 = jnp.bfloat16


def step_kernel(
    sizes,
    coef_hbm, sums_hbm, link_hbm, starts_hbm, ids_hbm, weight_hbm, dosage_hbm,
    updated_hbm, score_ref,
    coef, sums, link, starts_ref, ids_ref, weight_ref, dosage, low, ext, extf, peers, proposal, updated, updated_t, row,
    stats_out, stats_in, side_out, side_in, part_out, part_in,
    load_sem, link_sem, store_sem,
    halo_send, halo_recv, anc_send, anc_recv, stats_send, stats_recv, side_send, side_recv, part_send, part_recv,
):
    genomes, ancs, traits_n, reach, tile, groups = sizes
    traits_here, snps = coef.shape
    width = link.shape[1]
    tiles = snps // tile
    persons_per = part_out.shape[1]
    g = lax.axis_index("genome")
    a = lax.axis_index("anc")
    t = lax.axis_index("trait")
    stat_peers = [(k, m) for m in range(traits_n) for k in range(genomes) if (k, m) != (0, 0)]

    def genome_peer(k):
        return lax.rem(g + k, genomes)

    load_coef = pltpu.make_async_copy(coef_hbm.at[0], coef, load_sem.at[0])
    load_coef.start()
    barrier = pltpu.get_barrier_semaphore()
    for k, m in stat_peers:
        pl.semaphore_signal(
            barrier, inc=1, device_id_type=MESH,
            device_id={"genome": genome_peer(k), "trait": lax.rem(t + m, traits_n)},
        )
    for k in range(1, ancs):
        pl.semaphore_signal(
            barrier, inc=1, device_id={"anc": lax.rem(a + k, ancs)}, device_id_type=MESH
        )
    load_sums = pltpu.make_async_copy(sums_hbm.at[0], sums, load_sem.at[1])
    load_sums.start()
    load_small = [
        pltpu.make_async_copy(starts_hbm, starts_ref, load_sem.at[3]),
        pltpu.make_async_copy(ids_hbm, ids_ref, load_sem.at[4]),
        pltpu.make_async_copy(weight_hbm, weight_ref, load_sem.at[5]),
    ]
    for load in load_small:
        load.start()
    load_dosage = pltpu.make_async_copy(dosage_hbm.at[0], dosage, load_sem.at[2])

    def link_copy(u):
        rows = pl.ds(pl.multiple_of(u * tile, tile), tile)
        return pltpu.make_async_copy(link_hbm.at[0, rows, :], link.at[rows, :], link_sem.at[u])

    load_coef.wait()

    half = snps // 2
    even = 1 - 2 * lax.rem(g, 2)
    near, far, across = g + even, g + 2 * even, g - even

    def in_range(p):
        return jnp.logical_and(p >= 0, p < genomes)

    def own_block(u, carry):
        cols = pl.ds(pl.multiple_of(u * tile, tile), tile)
        block = coef[:, cols].astype(BF16)
        low[:, cols] = block
        flat = block.astype(F32).T
        extf[pl.ds(pl.multiple_of(reach * snps + u * tile, tile), tile), :] = flat
        ext[reach, cols, :] = flat.astype(BF16)
        return carry

    def halo_copy(src_slot, dst_slot, h, peer, send):
        rows = pl.ds(h * half, half)
        return pltpu.make_async_remote_copy(
            src_ref=ext.at[src_slot, rows, :], dst_ref=ext.at[dst_slot, rows, :],
            send_sem=halo_send.at[send], recv_sem=halo_recv.at[dst_slot, h],
            device_id={"genome": jnp.clip(peer, 0, genomes - 1)}, device_id_type=MESH,
        )

    def near_copy(h):
        return halo_copy(reach, reach - even, h, near, h)

    def far_copy(d, h):
        return halo_copy(reach, reach - d, h, g + d, (2 if d > 0 else 4) + h)

    def relay_far():
        return halo_copy(reach + even, reach - even, 0, far, 6)

    def relay_near():
        return halo_copy(reach + 2 * even, reach + even, 1, near, 7)

    def arrived(slot, h):
        halo_copy(reach, slot, h, near, 0).wait_recv()

    def anc_copy(k):
        return pltpu.make_async_remote_copy(
            src_ref=low, dst_ref=peers.at[k - 1],
            send_sem=anc_send.at[k - 1], recv_sem=anc_recv.at[k - 1],
            device_id={"anc": lax.rem(a + k, ancs)}, device_id_type=MESH,
        )

    def far_each(h):
        for d in (2, -2):
            @pl.when(in_range(g + d))
            def _(d=d):
                far_copy(d, h).start()

    lax.fori_loop(0, tiles // 2, own_block, 0, unroll=2)
    pl.semaphore_wait(barrier, len(stat_peers) + ancs - 1)
    near_copy(0).start()
    lax.fori_loop(tiles // 2, tiles, own_block, 0, unroll=2)
    far_each(1)
    near_copy(1).start()
    far_each(0)
    for k in range(1, ancs):
        anc_copy(k).start()
    for u in range(tiles):
        link_copy(u).start()
    load_dosage.start()

    chunk = 256

    def widen(slot, h):
        def piece(i, carry):
            at = pl.multiple_of(h * half + i * chunk, chunk)
            extf[pl.ds(pl.multiple_of(slot * snps + at, chunk), chunk), :] = (
                ext[slot, pl.ds(at, chunk), :].astype(F32)
            )
            return carry

        lax.fori_loop(0, half // chunk, piece, 0, unroll=2)

    for d in (-2, -1, 1, 2):
        @pl.when(jnp.logical_not(in_range(g + d)))
        def _(slot=reach + d):
            def clear(i, carry):
                at = pl.multiple_of(slot * snps + i * chunk, chunk)
                extf[pl.ds(at, chunk), :] = jnp.zeros((chunk, traits_here), F32)
                return carry

            lax.fori_loop(0, snps // chunk, clear, 0)

    arrived(reach + even, 0)

    @pl.when(in_range(far))
    def _():
        relay_far().start()
        arrived(reach + 2 * even, 1)
        relay_near().start()

    widen(reach + even, 0)

    @pl.when(in_range(far))
    def _():
        widen(reach + 2 * even, 1)

    @pl.when(in_range(g - 2 * even))
    def _():
        arrived(reach - 2 * even, 1)
        widen(reach - 2 * even, 1)

    arrived(reach + even, 1)
    widen(reach + even, 1)

    @pl.when(in_range(far))
    def _():
        arrived(reach + 2 * even, 0)
        widen(reach + 2 * even, 0)

    @pl.when(in_range(g - 2 * even))
    def _():
        arrived(reach - 2 * even, 0)
        widen(reach - 2 * even, 0)

    @pl.when(in_range(across))
    def _():
        for h in range(2):
            arrived(reach - even, h)
            widen(reach - even, h)

    load_sums.wait()
    for load in load_small:
        load.wait()

    def band_tile(u, carry):
        link_copy(u).wait()
        rows = pl.ds(pl.multiple_of(u * tile, tile), tile)
        begin = jnp.clip(starts_ref[0, u] - g * snps + reach * snps, 0, extf.shape[0] - width)
        depth = 512
        total = jnp.zeros((tile, traits_here), F32)
        for c in range(0, width, depth):
            window = extf[pl.ds(begin + c, depth), :].astype(BF16)
            total = total + jnp.dot(
                link[rows, c:c + depth], window, preferred_element_type=F32
            )
        band = total.T
        current = coef[:, rows]
        proposal[:, rows] = current + band - sums[:, rows]
        return carry

    lax.fori_loop(0, tiles, band_tile, 0, unroll=2)
    for k in range(1, ancs):
        anc_copy(k).wait_recv()

    def propose(u, carry):
        cols = pl.ds(pl.multiple_of(u * tile, tile), tile)
        current = coef[:, cols]
        mean = current
        for k in range(1, ancs):
            mean = mean + peers[k - 1, :, cols].astype(F32)
        mean = mean / ancs
        gradient = proposal[:, cols] + merging * (current - mean)
        value = current - step_size * gradient
        proposal[:, cols] = value
        row[:, cols] = jnp.sum(value * value, axis=0, keepdims=True)
        return carry

    lax.fori_loop(0, tiles, propose, 0, unroll=2)

    group_of = lax.broadcasted_iota(jnp.int32, (groups, snps), 0)
    mine = group_of == ids_ref[...]
    squares = jnp.sum(jnp.where(mine, row[...], 0.0), axis=1, keepdims=True)
    counts = jnp.sum(jnp.where(mine, 1.0, 0.0), axis=1, keepdims=True)
    lane = lax.broadcasted_iota(jnp.int32, (groups, 128), 1)
    stats = jnp.where(lane == 0, squares, jnp.where(lane == 1, counts, 0.0))
    stats_out[...] = stats

    def stats_copy(i):
        k, m = stat_peers[i]
        return pltpu.make_async_remote_copy(
            src_ref=stats_out, dst_ref=stats_in.at[i],
            send_sem=stats_send.at[i], recv_sem=stats_recv.at[i],
            device_id={"genome": genome_peer(k), "trait": lax.rem(t + m, traits_n)},
            device_id_type=MESH,
        )

    for i in range(len(stat_peers)):
        stats_copy(i).start()
    load_dosage.wait()
    for i in range(len(stat_peers)):
        stats_copy(i).wait_recv()
        stats = stats + stats_in[i]
    all_squares = stats[:, 0:1]
    all_counts = stats[:, 1:2] / traits_n
    square_of = lax.broadcasted_iota(jnp.int32, (groups, groups), 0)
    lane_of = lax.broadcasted_iota(jnp.int32, (groups, groups), 1)
    weight = jnp.sum(
        jnp.where(square_of == lane_of, weight_ref[...], 0.0), axis=1, keepdims=True
    )
    threshold = step_size * weight * jnp.sqrt(all_counts * (traits_here * traits_n))
    shrink = jnp.maximum(0.0, 1.0 - threshold / jnp.sqrt(all_squares + epsilon))
    row[...] = jnp.sum(jnp.where(mine, shrink, 0.0), axis=0, keepdims=True)

    def shrink_tile(u, carry):
        cols = pl.ds(pl.multiple_of(u * tile, tile), tile)
        value = proposal[:, cols] * row[:, cols]
        updated[:, cols] = value
        updated_t[cols, :] = value.T.astype(BF16)
        return carry

    lax.fori_loop(0, tiles, shrink_tile, 0, unroll=2)
    store = pltpu.make_async_copy(updated, updated_hbm.at[0], store_sem)
    store.start()

    scale = 1.0 / math.sqrt(snps * genomes)

    pairs = genomes // 2
    own_side, other_side = lax.rem(g, 2), lax.rem(near, 2)

    def pair_at(i):
        k = pairs // 2 + (1 - 2 * lax.rem(i, 2)) * ((i + 1) // 2)
        return lax.rem(g // 2 + k + pairs, pairs)

    def partial(person):
        at = pl.ds(pl.multiple_of(person * persons_per, persons_per), persons_per)
        return jnp.dot(dosage[at, :], updated_t[...], preferred_element_type=F32) * scale

    def side_copy(i):
        return pltpu.make_async_remote_copy(
            src_ref=side_out.at[i], dst_ref=side_in.at[i],
            send_sem=side_send.at[i], recv_sem=side_recv.at[i],
            device_id={"genome": near}, device_id_type=MESH,
        )

    def part_copy(i):
        return pltpu.make_async_remote_copy(
            src_ref=part_out.at[i], dst_ref=part_in.at[i],
            send_sem=part_send.at[i], recv_sem=part_recv.at[i],
            device_id={"genome": 2 * pair_at(i) + own_side}, device_id_type=MESH,
        )

    def send_side(i, carry):
        side_out[i] = partial(2 * pair_at(i) + other_side).astype(BF16)
        side_copy(i).start()
        return carry

    def pair_sum(i):
        mine_here = partial(2 * pair_at(i) + own_side)
        side_copy(i).wait_recv()
        return mine_here + side_in[i].astype(F32)

    def send_part(i, carry):
        part_out[i] = pair_sum(i).astype(BF16)
        part_copy(i).start()
        return carry

    lax.fori_loop(0, pairs, send_side, 0)
    lax.fori_loop(0, pairs - 1, send_part, 0)

    def add_part(i, total):
        part_copy(i).wait_recv()
        return total + part_in[i].astype(F32)

    score_ref[0] = lax.fori_loop(0, pairs - 1, add_part, pair_sum(pairs - 1)).T

    store.wait()
    for h in range(2):
        near_copy(h).wait_send()
        for d in (2, -2):
            @pl.when(in_range(g + d))
            def _(d=d, h=h):
                far_copy(d, h).wait_send()

    @pl.when(in_range(far))
    def _():
        relay_far().wait_send()
        relay_near().wait_send()

    for k in range(1, ancs):
        anc_copy(k).wait_send()
    for i in range(len(stat_peers)):
        stats_copy(i).wait_send()

    def sent_side(i, carry):
        side_copy(i).wait_send()
        return carry

    def sent_part(i, carry):
        part_copy(i).wait_send()
        return carry

    lax.fori_loop(0, pairs, sent_side, 0)
    lax.fori_loop(0, pairs - 1, sent_part, 0)


def per_device(coefficients, sumstats, linkage, band_start, group_ids, group_weight, dosage):
    _, traits_here, snps = coefficients.shape
    width = linkage.shape[2]
    genomes = lax.axis_size("genome")
    ancs = lax.axis_size("anc")
    traits_n = lax.axis_size("trait")
    persons = dosage.shape[1]
    persons_per = persons // genomes
    groups = group_weight.shape[1]
    reach = -(-width // snps)
    assert reach == 2 and genomes % 2 == 0 and coefficients.shape[0] == 1
    tile = snps // band_start.shape[1]
    slots = 2 * reach + 1
    pairs = genomes // 2
    stat_n = genomes * traits_n - 1
    sizes = (genomes, ancs, traits_n, reach, tile, groups)
    anyspace = pl.BlockSpec(memory_space=pl.ANY)
    hbm = pl.BlockSpec(memory_space=pltpu.HBM)
    vmem = pl.BlockSpec(memory_space=pltpu.VMEM)
    dma = pltpu.SemaphoreType.DMA
    return pl.pallas_call(
        functools.partial(step_kernel, sizes),
        out_shape=(
            jax.ShapeDtypeStruct((1, traits_here, snps), F32),
            jax.ShapeDtypeStruct((1, traits_here, persons_per), F32),
        ),
        in_specs=[hbm] * 7,
        out_specs=(anyspace, vmem),
        scratch_shapes=[
            pltpu.VMEM((traits_here, snps), F32),
            pltpu.VMEM((traits_here, snps), F32),
            pltpu.VMEM((snps, width), BF16),
            pltpu.SMEM(band_start.shape, jnp.int32),
            pltpu.VMEM(group_ids.shape, jnp.int32),
            pltpu.VMEM(group_weight.shape, F32),
            pltpu.VMEM((persons, snps), BF16),
            pltpu.VMEM((traits_here, snps), BF16),
            pltpu.VMEM((slots, snps, traits_here), BF16),
            pltpu.VMEM((slots * snps, traits_here), F32),
            pltpu.VMEM((ancs - 1, traits_here, snps), BF16),
            pltpu.VMEM((traits_here, snps), F32),
            pltpu.VMEM((traits_here, snps), F32),
            pltpu.VMEM((snps, traits_here), BF16),
            pltpu.VMEM((1, snps), F32),
            pltpu.VMEM((groups, 128), F32),
            pltpu.VMEM((stat_n, groups, 128), F32),
            pltpu.VMEM((pairs, persons_per, traits_here), BF16),
            pltpu.VMEM((pairs, persons_per, traits_here), BF16),
            pltpu.VMEM((pairs - 1, persons_per, traits_here), BF16),
            pltpu.VMEM((pairs - 1, persons_per, traits_here), BF16),
            dma((6,)), dma((snps // tile,)), dma,
            dma((8,)), dma((slots, 2)), dma((ancs - 1,)), dma((ancs - 1,)),
            dma((stat_n,)), dma((stat_n,)), dma((pairs,)), dma((pairs,)), dma((pairs - 1,)), dma((pairs - 1,)),
        ],
        compiler_params=pltpu.CompilerParams(
            collective_id=0, has_side_effects=True, vmem_limit_bytes=52 * 1024 * 1024
        ),
    )(coefficients, sumstats, linkage, band_start, group_ids, group_weight, dosage)


def solution(mesh):
    in_specs = (
        P("anc", "trait", "genome"),
        P("anc", "trait", "genome"),
        P("anc", "genome", None),
        P("anc", "genome"),
        P("anc", "genome"),
        P("anc", None),
        P("anc", None, "genome"),
    )
    out_specs = (P("anc", "trait", "genome"), P("anc", "trait", "genome"))
    return jax.shard_map(
        per_device, mesh=mesh, in_specs=in_specs, out_specs=out_specs, check_vma=False
    )
```
